32 devices in a mesh: ep: 16 (over z, y, x), dp: 2 (over core).
Axes of the slice: x: 2, y: 2, z: 4, core: 2. Of those that a mesh axis runs over, the one named last changes fastest.
Arguments:
- grad_out: bfloat16 [4096, 2048], P(('ep', 'dp')), may hold values from -6 to 6
- router_prob: bfloat16 [4096], P(('ep', 'dp')), may hold values from 0.19921875 to 1
- routes: int32 [4096, 1], P(('ep', 'dp')), may hold values from 0 to 63, as said below
- token_inputs: bfloat16 [4096, 2048], P(('ep', 'dp')), may hold values from -6 to 6
- w_in: bfloat16 [7168, 2048], P(('ep', 'dp')), may hold values from -0.125 to 0.125
- w_out: bfloat16 [7168, 2048], P(('ep', 'dp')), may hold values from -0.0625 to 0.0625
Outputs:
- grad_tokens: bfloat16 [4096, 2048], P(('ep', 'dp'))
- grad_in_weight: bfloat16 [7168, 2048], P(('ep', 'dp'))
- grad_out_weight: bfloat16 [7168, 2048], P(('ep', 'dp'))
The draws below stay inside these ranges and needn't reach their ends.
Inputs may be any that keep to these rules, and one draw needn't show every extreme that they name: `routes`: ids below 1 are the experts of this window; the rows of one device name each of them at most 3 times, and in every draw one of them is named exactly 3 times by the rows of every device of one dp index.
All inputs are finite; a program needn't handle non-finite values.
Results may differ from the reference program's by a relative error of at most 0.014.
Values may be sent and summed in bfloat16 or wider, within the bound.
A program may use at most 64 MiB of HBM per device.

```python
import math
import jax
import jax.numpy as jnp
from jax import lax

D = 2048
EXPERT_FF = 7168
EXPERTS = 64
GROUP = 16
CAP = 3
TOK_DEV = 128
FLIGHT = 1
SLOTS = 48
REPLICAS = 2
TOKENS = 4096


def shuffle_row(row_key, row_values):
    return jax.random.permutation(row_key, row_values)


def draw_routes(key, part):
    blocks = TOKENS // TOK_DEV
    key_count, key_hot, key_other, key_order = jax.random.split(key, 4)
    counts = jax.random.randint(key_count, (blocks, FLIGHT), 0, CAP + 1)
    hot_rows = jax.random.randint(key_hot, (REPLICAS,), 0, FLIGHT)
    block_ids = jnp.arange(blocks, dtype=jnp.int32)
    hottest = hot_rows[block_ids % REPLICAS]
    counts = jnp.where(jnp.arange(FLIGHT, dtype=jnp.int32)[None, :] == hottest[:, None], CAP, counts)
    bounds = jnp.cumsum(counts, axis=1)
    position = jnp.arange(TOK_DEV, dtype=jnp.int32)
    chosen = jnp.sum((position[None, :, None] >= bounds[:, None, :]).astype(jnp.int32), axis=2)
    others = FLIGHT + jax.random.randint(key_other, (blocks, TOK_DEV), 0, EXPERTS - FLIGHT)
    chosen = jnp.where(chosen < FLIGHT, chosen, others)
    order_keys = jax.random.split(key_order, blocks)
    shuffled = jax.vmap(shuffle_row)(order_keys, chosen)
    return shuffled.reshape(TOKENS, 1).astype(jnp.int32)


def block_levels(key, shape, pieces, low, largest):
    def one(axis_at, shards_of):
        draws = jax.random.uniform(jax.random.fold_in(jax.random.fold_in(key, 6), axis_at), (shards_of,), jnp.float32, low / len(pieces), largest / len(pieces))
        return jnp.repeat(jnp.exp(draws), shape[axis_at] // shards_of).reshape((-1,) + (1,) * (len(shape) - axis_at - 1))

    loudness = one(*pieces[0])
    for cut in pieces[1:]:
        loudness = loudness * one(*cut)
    return loudness


def noise(key, extent, spread, bound, cuts=(), held_as=jnp.bfloat16):
    drawn = jax.random.normal(key, extent, jnp.float32) * spread
    if len(cuts) > 0:
        drawn = block_levels(key, extent, cuts, -0.22, 0.18) * drawn
    return jnp.clip(drawn, min=-bound, max=bound).astype(held_as)


def setup_inputs(seed: int = 0) -> dict:
    key_of = jax.random.split(jax.random.key(seed), 7)
    grad_out = noise(key_of[0], (TOKENS, D), 1.0, 6.0, ((0, 32),))
    router_prob = jnp.clip(0.19921875 + 0.80078125 * jax.random.uniform(key_of[1], (TOKENS,), jnp.float32) ** block_levels(key_of[1], (TOKENS,), ((0, 32),), -0.2, 0.2), 0.19921875, 1.0).astype(jnp.bfloat16)
    routes = draw_routes(jax.random.fold_in(key_of[6], 71), 0)
    token_inputs = noise(key_of[3], (TOKENS, D), 1.0, 6.0, ((0, 32),))
    w_in = noise(key_of[4], (FLIGHT * EXPERT_FF, D), D ** -0.5, 0.125, ((0, 32),))
    w_out = noise(key_of[5], (FLIGHT * EXPERT_FF, D), EXPERT_FF ** -0.5, 0.0625, ((0, 32),))
    return {"grad_out": grad_out, "router_prob": router_prob, "routes": routes, "token_inputs": token_inputs, "w_in": w_in, "w_out": w_out}


def slot_rows(routes):
    blocks = TOKENS // TOK_DEV
    chosen = routes[:, 0].reshape(blocks, TOK_DEV)
    onehot = (chosen[:, :, None] == jnp.arange(FLIGHT, dtype=jnp.int32)[None, None, :]).astype(jnp.int32)
    before = jnp.cumsum(onehot, axis=1) - onehot
    slot_rank = lax.optimization_barrier(jnp.sum(before * onehot, axis=2))
    block_ids = jnp.arange(blocks, dtype=jnp.int32)[:, None]
    source = block_ids // REPLICAS
    replica = block_ids % REPLICAS
    in_window = chosen < FLIGHT
    dest_rows = (chosen * REPLICAS + replica) * SLOTS + source * CAP + slot_rank
    all_rows = FLIGHT * REPLICAS * SLOTS
    dest_rows = jnp.where(in_window, dest_rows, all_rows)
    return (dest_rows.reshape(-1).astype(jnp.int32), in_window.reshape(-1))

def reference(grad_out, router_prob, routes, token_inputs, w_in, w_out):
    dest_rows, in_window = slot_rows(routes)
    all_rows = FLIGHT * REPLICAS * SLOTS
    scaled = (router_prob.astype(jnp.float32)[:, None] * grad_out.astype(jnp.float32)).astype(jnp.bfloat16)
    dispatched = jnp.zeros((all_rows, D), jnp.bfloat16).at[dest_rows].set(scaled, mode='drop')
    gathered_inputs = jnp.zeros((all_rows, D), jnp.bfloat16).at[dest_rows].set(token_inputs, mode='drop')
    group_inputs = gathered_inputs.reshape(FLIGHT, REPLICAS, SLOTS, D)
    group_grads = dispatched.reshape(FLIGHT, REPLICAS, SLOTS, D)
    weights_in = w_in.reshape(FLIGHT, EXPERT_FF, D)
    weights_out = w_out.reshape(FLIGHT, EXPERT_FF, D)
    grad_scale = 1.0 / math.sqrt(REPLICAS * SLOTS)
    piece_size = EXPERT_FF // GROUP

    def one_expert(operands):
        inputs, slot_grads, weight_in, weight_out = operands
        weight_pieces = weight_in.reshape(GROUP, piece_size, D)

        def one_replica(pair):
            rows_in, cotangent = pair
            pre_act = jnp.dot(rows_in, weight_in.T, preferred_element_type=jnp.float32)
            gate_sig = jax.nn.sigmoid(pre_act)
            hidden = (pre_act * gate_sig).astype(jnp.bfloat16)
            back_prop = jnp.dot(cotangent, weight_out.T, preferred_element_type=jnp.float32)
            grad_pre = (back_prop * gate_sig * (1.0 + pre_act * (1.0 - gate_sig))).astype(jnp.bfloat16)
            grad_pieces = jnp.transpose(grad_pre.reshape(SLOTS, GROUP, piece_size), (1, 0, 2))

            def add_piece(total, items):
                grad_piece, weight_piece = items
                piece_grad = jnp.dot(grad_piece, weight_piece, preferred_element_type=jnp.float32).astype(jnp.bfloat16)
                piece_grad = lax.optimization_barrier(piece_grad).astype(jnp.float32)
                return (total + piece_grad, None)
            slot_grad, unused = lax.scan(add_piece, jnp.zeros((SLOTS, D), jnp.float32), (grad_pieces, weight_pieces))
            part_in = jnp.dot(grad_pre.T, rows_in, preferred_element_type=jnp.float32).astype(jnp.bfloat16)
            part_out = jnp.dot(hidden.T, cotangent, preferred_element_type=jnp.float32).astype(jnp.bfloat16)
            part_in = lax.optimization_barrier(part_in).astype(jnp.float32)
            part_out = lax.optimization_barrier(part_out).astype(jnp.float32)
            return (slot_grad, part_in, part_out)
        slot_grad, part_in, part_out = lax.map(one_replica, (inputs, slot_grads))
        grad_in = (lax.optimization_barrier(jnp.sum(part_in, axis=0)) * grad_scale).astype(jnp.bfloat16)
        grad_outw = (lax.optimization_barrier(jnp.sum(part_out, axis=0)) * grad_scale).astype(jnp.bfloat16)
        return (slot_grad, grad_in, grad_outw)
    slot_grad, grad_in, grad_outw = lax.map(one_expert, (group_inputs, group_grads, weights_in, weights_out))
    flat_grad = slot_grad.reshape(all_rows, D)
    picked = flat_grad[jnp.minimum(dest_rows, all_rows - 1).astype(jnp.int32)]
    grad_tokens = jnp.where(in_window[:, None], picked, jnp.float32(0.0)).astype(jnp.bfloat16)
    return (grad_tokens, grad_in.reshape(FLIGHT * EXPERT_FF, D), grad_outw.reshape(FLIGHT * EXPERT_FF, D))
```

```python
import functools
import math

import jax
import jax.numpy as jnp
from jax import lax
from jax.experimental import pallas as pl
from jax.experimental.pallas import tpu as pltpu
from jax.sharding import PartitionSpec as P

GROUP = 16
CAP = 3
LINES = 8
LANES = 128
MESH = pl.DeviceIdType.MESH


def per_device(grad_out, router_prob, routes, token_inputs, w_in, w_out):
    ep_count = lax.axis_size("ep")
    replicas = lax.axis_size("dp")
    flight = ep_count // GROUP
    tok_rows = grad_out.shape[0]
    model_width = grad_out.shape[1]
    expert_ids = routes[:, 0]
    in_window = expert_ids < flight
    onehot = (expert_ids[:, None] == jnp.arange(flight, dtype=jnp.int32)[None, :]).astype(
        jnp.bfloat16
    )
    earlier = (
        jnp.arange(tok_rows, dtype=jnp.int32)[:, None]
        > jnp.arange(tok_rows, dtype=jnp.int32)[None, :]
    ).astype(jnp.bfloat16)
    before = jnp.dot(earlier, onehot, preferred_element_type=jnp.float32)
    slot_rank = jnp.sum(before * onehot.astype(jnp.float32), axis=1).astype(jnp.int32)
    window_rows = flight * CAP
    target = jnp.where(in_window, expert_ids * CAP + slot_rank, window_rows)
    chooser = (jnp.arange(window_rows, dtype=jnp.int32)[:, None] == target[None, :]).astype(
        jnp.bfloat16
    )
    scaled = (router_prob.astype(jnp.float32)[:, None] * grad_out.astype(jnp.float32)).astype(
        jnp.bfloat16
    )
    paired = jnp.concatenate((scaled, token_inputs), axis=1)
    outgoing = jnp.dot(chooser, paired, preferred_element_type=jnp.float32).astype(jnp.bfloat16)
    outgoing = jnp.broadcast_to(
        outgoing.reshape(flight, 1, CAP, 2 * model_width), (flight, GROUP, CAP, 2 * model_width)
    )
    outgoing = outgoing.reshape(ep_count, CAP, 2 * model_width)
    incoming = lax.all_to_all(outgoing, "ep", split_axis=0, concat_axis=0, tiled=True)
    slot_total = ep_count * CAP
    incoming = incoming.reshape(slot_total, 2 * model_width)
    cotangent = incoming[:, :model_width]
    rows_in = incoming[:, model_width:]
    weight_in, weight_out = (
        lax.all_gather(w_in, "dp", axis=0, tiled=True),
        lax.all_gather(w_out, "dp", axis=0, tiled=True),
    )
    contract_last = (((1,), (1,)), ((), ()))
    contract_first = (((0,), (0,)), ((), ()))
    pre_act = lax.dot_general(rows_in, weight_in, contract_last, preferred_element_type=jnp.float32)
    gate_sig = jax.nn.sigmoid(pre_act)
    hidden = (pre_act * gate_sig).astype(jnp.bfloat16)
    back_prop = lax.dot_general(
        cotangent, weight_out, contract_last, preferred_element_type=jnp.float32
    )
    grad_pre = (back_prop * gate_sig * (1.0 + pre_act * (1.0 - gate_sig))).astype(jnp.bfloat16)
    piece_grad = jnp.dot(grad_pre, weight_in, preferred_element_type=jnp.float32).astype(
        jnp.bfloat16
    )
    piece_grad = piece_grad.reshape(ep_count, CAP, model_width)
    returned = lax.all_to_all(piece_grad, "ep", split_axis=0, concat_axis=0, tiled=True)
    summed = jnp.sum(returned.reshape(flight, GROUP, CAP, model_width).astype(jnp.float32), axis=1)
    summed = summed.reshape(window_rows, model_width)
    picked = jnp.take(summed, jnp.minimum(target, window_rows - 1), axis=0)
    grad_tokens = jnp.where(in_window[:, None], picked, jnp.float32(0.0)).astype(jnp.bfloat16)
    grad_scale = 1.0 / math.sqrt(replicas * slot_total)
    columns = grad_pre
    grad_in = lax.psum_scatter(
        lax.dot_general(
            columns, rows_in, contract_first, preferred_element_type=jnp.float32
        ).astype(jnp.bfloat16),
        "dp",
        scatter_dimension=0,
        tiled=True,
    ).astype(jnp.float32)
    columns = hidden
    grad_outw = lax.psum_scatter(
        lax.dot_general(
            columns, cotangent, contract_first, preferred_element_type=jnp.float32
        ).astype(jnp.bfloat16),
        "dp",
        scatter_dimension=0,
        tiled=True,
    ).astype(jnp.float32)
    return (
        grad_tokens,
        (grad_in * grad_scale).astype(jnp.bfloat16),
        (grad_outw * grad_scale).astype(jnp.bfloat16),
    )


def fused_kernel(
    n,
    inner,
    grad_out,
    prob,
    routes,
    tokens,
    w_in,
    w_out,
    tok_out,
    gin_out,
    gout_out,
    go_v,
    ti_v,
    wi_v,
    wo_v,
    recv,
    x32,
    q_b,
    x_b,
    hid_v,
    gp_v,
    ret32,
    ret_send,
    ret_recv,
    d_send,
    d_recv,
    g_v,
    tok_v,
    load_sem,
    w_send,
    w_recv,
    a_send,
    a_recv,
    r_send,
    r_recv,
    d_ssem,
    d_rsem,
    out_sem,
):
    me = lax.axis_index("ep")
    core = lax.axis_index("dp")
    partner = 1 - core
    outer = n // inner
    o, i = me // inner, me % inner
    rows, width = w_in.shape
    tok_rows = tokens.shape[0]
    block_rows = CAP * LINES
    half = LINES // 2
    wide = 2 * width // LINES
    narrow = width // LINES
    slots = n * CAP
    f32, bf16 = jnp.float32, jnp.bfloat16

    def to(src, dst, send, arrive, ep, dp):
        return pltpu.make_async_remote_copy(
            src_ref=src,
            dst_ref=dst,
            send_sem=send,
            recv_sem=arrive,
            device_id=(ep, dp),
            device_id_type=MESH,
        )

    barrier = pltpu.get_barrier_semaphore()
    for k in range(1, n):
        pl.semaphore_signal(barrier, inc=1, device_id=((me + k) % n, core), device_id_type=MESH)
    pl.semaphore_signal(barrier, inc=1, device_id=(me, partner), device_id_type=MESH)

    load_go = pltpu.make_async_copy(grad_out, go_v, load_sem.at[0])
    load_ti = pltpu.make_async_copy(tokens, ti_v, load_sem.at[1])
    mine = pl.ds(pl.multiple_of(core * rows, rows), rows)
    theirs = pl.ds(pl.multiple_of(partner * rows, rows), rows)
    load_wi = pltpu.make_async_copy(w_in, wi_v.at[mine], load_sem.at[2])
    load_wo = pltpu.make_async_copy(w_out, wo_v.at[mine], load_sem.at[3])
    load_go.start()
    load_ti.start()
    load_wi.start()
    load_wo.start()

    line = lax.broadcasted_iota(jnp.int32, (block_rows, tok_rows), 0)
    in_window = jnp.broadcast_to((routes[...] < 1).astype(f32), (block_rows, tok_rows))
    earlier = (
        lax.broadcasted_iota(jnp.int32, (tok_rows, tok_rows), 0)
        < lax.broadcasted_iota(jnp.int32, (tok_rows, tok_rows), 1)
    ).astype(f32).astype(bf16)
    rank = jnp.dot(in_window.astype(bf16), earlier, preferred_element_type=f32)
    rank_of_line = (line // LINES).astype(f32)
    sel = jnp.where(rank == rank_of_line, in_window, 0.0)
    weight = jnp.sum(sel * prob[...].astype(f32), axis=1, keepdims=True)
    lane_of = line % LINES
    weight = jnp.where(lane_of[:, :1] < half, weight, 1.0)
    load_go.wait()
    load_ti.wait()
    block = jnp.zeros((block_rows, wide), f32)
    for g in range(LINES):
        picked = jnp.where(lane_of == g, sel, 0.0).astype(bf16)
        source = go_v if g < half else ti_v
        columns = pl.ds((g % half) * wide, wide)
        block += jnp.dot(picked, source[:, columns], preferred_element_type=f32)
    recv[me] = (block * weight).astype(bf16)
    pl.semaphore_wait(barrier, n)

    sends = []

    def spread(b, ep):
        copy = to(recv.at[b], recv.at[b], a_send.at[len(sends)], a_recv.at[b], ep, core)
        copy.start()
        sends.append(copy)

    def arrived(b):
        to(recv.at[b], recv.at[b], a_send.at[0], a_recv.at[b], me, partner).wait_recv()

    def unpack(b):
        at = pl.ds(pl.multiple_of(b * block_rows, LINES), block_rows)
        for c in range(wide // LANES):
            x32[c, at, :] = recv[b, :, pl.ds(c * LANES, LANES)].astype(f32)

    for k in range(outer - 1, 0, -1):
        spread(me, ((o + k) % outer) * inner + i)
    for j in range(1, inner):
        spread(me, o * inner + (i + j) % inner)
    push_wi = to(w_in, wi_v.at[mine], w_send.at[0], w_recv.at[0], me, partner)
    push_wo = to(w_out, wo_v.at[mine], w_send.at[1], w_recv.at[1], me, partner)
    push_wi.start()
    push_wo.start()
    unpack(me)
    for k in range(1, outer):
        b = ((o + outer - k) % outer) * inner + i
        arrived(b)
        for j in range(1, inner):
            spread(b, o * inner + (i + j) % inner)
        unpack(b)
    load_wi.wait()
    load_wo.wait()
    to(w_in, wi_v.at[theirs], w_send.at[0], w_recv.at[0], me, partner).wait_recv()
    to(w_out, wo_v.at[theirs], w_send.at[1], w_recv.at[1], me, partner).wait_recv()
    for k in range(outer):
        for j in range(1, inner):
            b = ((o + outer - k) % outer) * inner + (i + inner - j) % inner
            arrived(b)
            unpack(b)

    for g in range(LINES):
        dest = q_b if g < half else x_b
        for c in range(wide // LANES):
            columns = pl.ds((g % half) * wide + c * LANES, LANES)
            dest[:, columns] = x32[c, pl.ds(g, slots, stride=LINES), :].astype(bf16)

    last = (((1,), (1,)), ((), ()))
    pre = lax.dot_general(wi_v[...], x_b[...], last, preferred_element_type=f32)
    back = lax.dot_general(wo_v[...], q_b[...], last, preferred_element_type=f32)
    sig = jax.nn.sigmoid(pre)
    grad_pre = back * sig * (1.0 + pre * (1.0 - sig))
    gp_v[...] = grad_pre.astype(bf16)
    hid_v[...] = (pre * sig).astype(bf16)
    flat = grad_pre.T.astype(bf16)
    for g in range(LINES):
        piece = jnp.dot(flat, wi_v[:, pl.ds(g * narrow, narrow)], preferred_element_type=f32)
        for c in range(narrow // LANES):
            ret32[c, pl.ds(g, slots, stride=LINES), :] = piece[:, c * LANES : (c + 1) * LANES]
    for b in range(n):
        for c in range(narrow // LANES):
            ret_send[b, :, pl.ds(c * LANES, LANES)] = ret32[
                c, pl.ds(b * block_rows, block_rows), :
            ].astype(bf16)
    returns = []
    for k in range(n - 1, 0, -1):
        dst = (me + k) % n
        copy = to(ret_send.at[dst], ret_recv.at[me], r_send.at[k - 1], r_recv.at[me], dst, core)
        copy.start()
        returns.append(copy)

    chunk = 512
    swaps = []
    for w, (left, right) in enumerate(((gp_v, x_b), (hid_v, q_b))):
        for c in range(0, width, chunk):
            cols = pl.ds(c, chunk)
            d_send[w, :, cols] = jnp.dot(
                left[theirs, :], right[:, cols], preferred_element_type=f32
            ).astype(bf16)
        copy = to(d_send.at[w], d_recv.at[w], d_ssem.at[w], d_rsem.at[w], me, partner)
        copy.start()
        swaps.append(copy)
    grad_scale = 1.0 / math.sqrt(2 * slots)
    outs = []
    for w, (left, right, out) in enumerate(((gp_v, x_b, gin_out), (hid_v, q_b, gout_out))):
        swaps[w].wait_recv()
        for c in range(0, width, chunk):
            cols = pl.ds(c, chunk)
            own = jnp.dot(left[mine, :], right[:, cols], preferred_element_type=f32)
            total = own.astype(bf16).astype(f32) + d_recv[w, :, cols].astype(f32)
            g_v[w, :, cols] = (total * grad_scale).astype(bf16)
        copy = pltpu.make_async_copy(g_v.at[w], out, out_sem.at[w])
        copy.start()
        outs.append(copy)

    summed = ret_send[me].astype(f32)
    for k in range(1, n):
        b = (me + n - k) % n
        to(ret_send.at[b], ret_recv.at[b], r_send.at[0], r_recv.at[b], me, partner).wait_recv()
        summed += ret_recv[b].astype(f32)
    rounded = summed.astype(bf16)
    for g in range(LINES):
        picked = jnp.where(lane_of == g, sel, 0.0).T.astype(bf16)
        tok_v[:, pl.ds(g * narrow, narrow)] = jnp.dot(
            picked, rounded, preferred_element_type=f32
        ).astype(bf16)
    copy = pltpu.make_async_copy(tok_v, tok_out, out_sem.at[2])
    copy.start()
    outs.append(copy)
    for copy in sends + returns + swaps + [push_wi, push_wo]:
        copy.wait_send()
    for copy in outs:
        copy.wait()


def per_device_fused(grad_out, router_prob, routes, token_inputs, w_in, w_out):
    n = lax.axis_size("ep")
    inner = 1 << (n.bit_length() // 2)
    tok_rows, width = token_inputs.shape
    rows = w_in.shape[0]
    block_rows = CAP * LINES
    wide = 2 * width // LINES
    narrow = width // LINES
    slots = n * CAP
    f32, bf16 = jnp.float32, jnp.bfloat16
    copies = n - 1
    dma = pltpu.SemaphoreType.DMA
    anywhere = pl.BlockSpec(memory_space=pl.ANY)
    vmem = pl.BlockSpec(memory_space=pltpu.VMEM)
    return pl.pallas_call(
        functools.partial(fused_kernel, n, inner),
        out_shape=(
            jax.ShapeDtypeStruct((tok_rows, width), bf16),
            jax.ShapeDtypeStruct((rows, width), bf16),
            jax.ShapeDtypeStruct((rows, width), bf16),
        ),
        in_specs=[anywhere, vmem, vmem, anywhere, anywhere, anywhere],
        out_specs=(anywhere, anywhere, anywhere),
        scratch_shapes=[
            pltpu.VMEM((tok_rows, width), bf16),
            pltpu.VMEM((tok_rows, width), bf16),
            pltpu.VMEM((2 * rows, width), bf16),
            pltpu.VMEM((2 * rows, width), bf16),
            pltpu.VMEM((n, block_rows, wide), bf16),
            pltpu.VMEM((wide // LANES, n * block_rows, LANES), f32),
            pltpu.VMEM((slots, width), bf16),
            pltpu.VMEM((slots, width), bf16),
            pltpu.VMEM((2 * rows, slots), bf16),
            pltpu.VMEM((2 * rows, slots), bf16),
            pltpu.VMEM((narrow // LANES, n * block_rows, LANES), f32),
            pltpu.VMEM((n, block_rows, narrow), bf16),
            pltpu.VMEM((n, block_rows, narrow), bf16),
            pltpu.VMEM((2, rows, width), bf16),
            pltpu.VMEM((2, rows, width), bf16),
            pltpu.VMEM((2, rows, width), bf16),
            pltpu.VMEM((tok_rows, width), bf16),
            dma((4,)),
            dma((2,)),
            dma((2,)),
            dma((copies,)),
            dma((n,)),
            dma((copies,)),
            dma((n,)),
            dma((2,)),
            dma((2,)),
            dma((3,)),
        ],
        compiler_params=pltpu.CompilerParams(
            collective_id=0, has_side_effects=True, vmem_limit_bytes=40 * 1024 * 1024
        ),
    )(grad_out, router_prob.reshape(1, tok_rows), routes.reshape(1, tok_rows), token_inputs, w_in, w_out)


def solution(mesh):
    in_specs = (
        P(("ep", "dp"), None),
        P(("ep", "dp")),
        P(("ep", "dp"), None),
        P(("ep", "dp"), None),
        P(("ep", "dp"), None),
        P(("ep", "dp"), None),
    )
    out_specs = (P(("ep", "dp"), None), P(("ep", "dp"), None), P(("ep", "dp"), None))
    fused = mesh.shape["ep"] == GROUP and mesh.shape["dp"] == 2
    return jax.shard_map(
        per_device_fused if fused else per_device, mesh=mesh, in_specs=in_specs, out_specs=out_specs, check_vma=False
    )
```

```python
import functools
import math

import jax
import jax.numpy as jnp
from jax import lax
from jax.experimental import pallas as pl
from jax.experimental.pallas import tpu as pltpu
from jax.sharding import PartitionSpec as P

GROUP = 16
CAP = 3
LINES = 8
LANES = 128
MESH = pl.DeviceIdType.MESH


def per_device(grad_out, router_prob, routes, token_inputs, w_in, w_out):
    ep_count = lax.axis_size("ep")
    replicas = lax.axis_size("dp")
    flight = ep_count // GROUP
    tok_rows = grad_out.shape[0]
    model_width = grad_out.shape[1]
    expert_ids = routes[:, 0]
    in_window = expert_ids < flight
    onehot = (expert_ids[:, None] == jnp.arange(flight, dtype=jnp.int32)[None, :]).astype(
        jnp.bfloat16
    )
    earlier = (
        jnp.arange(tok_rows, dtype=jnp.int32)[:, None]
        > jnp.arange(tok_rows, dtype=jnp.int32)[None, :]
    ).astype(jnp.bfloat16)
    before = jnp.dot(earlier, onehot, preferred_element_type=jnp.float32)
    slot_rank = jnp.sum(before * onehot.astype(jnp.float32), axis=1).astype(jnp.int32)
    window_rows = flight * CAP
    target = jnp.where(in_window, expert_ids * CAP + slot_rank, window_rows)
    chooser = (jnp.arange(window_rows, dtype=jnp.int32)[:, None] == target[None, :]).astype(
        jnp.bfloat16
    )
    scaled = (router_prob.astype(jnp.float32)[:, None] * grad_out.astype(jnp.float32)).astype(
        jnp.bfloat16
    )
    paired = jnp.concatenate((scaled, token_inputs), axis=1)
    outgoing = jnp.dot(chooser, paired, preferred_element_type=jnp.float32).astype(jnp.bfloat16)
    outgoing = jnp.broadcast_to(
        outgoing.reshape(flight, 1, CAP, 2 * model_width), (flight, GROUP, CAP, 2 * model_width)
    )
    outgoing = outgoing.reshape(ep_count, CAP, 2 * model_width)
    incoming = lax.all_to_all(outgoing, "ep", split_axis=0, concat_axis=0, tiled=True)
    slot_total = ep_count * CAP
    incoming = incoming.reshape(slot_total, 2 * model_width)
    cotangent = incoming[:, :model_width]
    rows_in = incoming[:, model_width:]
    weight_in, weight_out = (
        lax.all_gather(w_in, "dp", axis=0, tiled=True),
        lax.all_gather(w_out, "dp", axis=0, tiled=True),
    )
    contract_last = (((1,), (1,)), ((), ()))
    contract_first = (((0,), (0,)), ((), ()))
    pre_act = lax.dot_general(rows_in, weight_in, contract_last, preferred_element_type=jnp.float32)
    gate_sig = jax.nn.sigmoid(pre_act)
    hidden = (pre_act * gate_sig).astype(jnp.bfloat16)
    back_prop = lax.dot_general(
        cotangent, weight_out, contract_last, preferred_element_type=jnp.float32
    )
    grad_pre = (back_prop * gate_sig * (1.0 + pre_act * (1.0 - gate_sig))).astype(jnp.bfloat16)
    piece_grad = jnp.dot(grad_pre, weight_in, preferred_element_type=jnp.float32).astype(
        jnp.bfloat16
    )
    piece_grad = piece_grad.reshape(ep_count, CAP, model_width)
    returned = lax.all_to_all(piece_grad, "ep", split_axis=0, concat_axis=0, tiled=True)
    summed = jnp.sum(returned.reshape(flight, GROUP, CAP, model_width).astype(jnp.float32), axis=1)
    summed = summed.reshape(window_rows, model_width)
    picked = jnp.take(summed, jnp.minimum(target, window_rows - 1), axis=0)
    grad_tokens = jnp.where(in_window[:, None], picked, jnp.float32(0.0)).astype(jnp.bfloat16)
    grad_scale = 1.0 / math.sqrt(replicas * slot_total)
    columns = grad_pre
    grad_in = lax.psum_scatter(
        lax.dot_general(
            columns, rows_in, contract_first, preferred_element_type=jnp.float32
        ).astype(jnp.bfloat16),
        "dp",
        scatter_dimension=0,
        tiled=True,
    ).astype(jnp.float32)
    columns = hidden
    grad_outw = lax.psum_scatter(
        lax.dot_general(
            columns, cotangent, contract_first, preferred_element_type=jnp.float32
        ).astype(jnp.bfloat16),
        "dp",
        scatter_dimension=0,
        tiled=True,
    ).astype(jnp.float32)
    return (
        grad_tokens,
        (grad_in * grad_scale).astype(jnp.bfloat16),
        (grad_outw * grad_scale).astype(jnp.bfloat16),
    )


def fused_kernel(
    n,
    inner,
    grad_out,
    prob,
    routes,
    tokens,
    w_in,
    w_out,
    tok_out,
    grads_out,
    go_v,
    ti_v,
    wi_v,
    wo_v,
    recv,
    x32,
    q_b,
    x_b,
    hid_v,
    gp_v,
    ret32,
    ret_send,
    ret_recv,
    d_send,
    d_recv,
    prob_v,
    routes_v,
    load_sem,
    w_send,
    w_recv,
    a_send,
    a_recv,
    r_send,
    r_recv,
    d_ssem,
    d_rsem,
):
    me = lax.axis_index("ep")
    core = lax.axis_index("dp")
    partner = 1 - core
    outer = n // inner
    o, i = me // inner, me % inner
    rows, width = w_in.shape
    tok_rows = tokens.shape[0]
    block_rows = CAP * LINES
    half = LINES // 2
    wide = 2 * width // LINES
    narrow = width // LINES
    slots = n * CAP
    f32, bf16 = jnp.float32, jnp.bfloat16

    def to(src, dst, send, arrive, ep, dp):
        return pltpu.make_async_remote_copy(
            src_ref=src,
            dst_ref=dst,
            send_sem=send,
            recv_sem=arrive,
            device_id=(ep, dp),
            device_id_type=MESH,
        )

    barrier = pltpu.get_barrier_semaphore()
    for k in range(1, outer):
        peer = ((o + k) % outer) * inner + i
        pl.semaphore_signal(barrier, inc=1, device_id=(peer, core), device_id_type=MESH)
    for j in range(1, inner):
        peer = o * inner + (i + j) % inner
        pl.semaphore_signal(barrier, inc=1, device_id=(peer, core), device_id_type=MESH)
    pl.semaphore_signal(barrier, inc=1, device_id=(me, partner), device_id_type=MESH)

    load_go = pltpu.make_async_copy(grad_out, go_v, load_sem.at[0])
    load_ti = pltpu.make_async_copy(tokens, ti_v, load_sem.at[1])
    mine = pl.ds(pl.multiple_of(core * rows, rows), rows)
    theirs = pl.ds(pl.multiple_of(partner * rows, rows), rows)
    load_wi = pltpu.make_async_copy(w_in, wi_v.at[mine], load_sem.at[2])
    load_wo = pltpu.make_async_copy(w_out, wo_v.at[mine], load_sem.at[3])
    load_prob = pltpu.make_async_copy(prob, prob_v, load_sem.at[4])
    load_routes = pltpu.make_async_copy(routes, routes_v, load_sem.at[5])
    load_routes.start()
    load_prob.start()
    load_go.start()
    load_ti.start()
    load_wi.start()
    load_wo.start()

    line = lax.broadcasted_iota(jnp.int32, (block_rows, tok_rows), 0)
    load_routes.wait()
    load_prob.wait()
    in_window = jnp.broadcast_to((routes_v[...] < 1).astype(f32), (block_rows, tok_rows))
    earlier = (
        lax.broadcasted_iota(jnp.int32, (tok_rows, tok_rows), 0)
        < lax.broadcasted_iota(jnp.int32, (tok_rows, tok_rows), 1)
    ).astype(f32).astype(bf16)
    rank = jnp.dot(in_window.astype(bf16), earlier, preferred_element_type=f32)
    rank_of_line = (line // LINES).astype(f32)
    sel = jnp.where(rank == rank_of_line, in_window, 0.0)
    weight = jnp.sum(sel * prob_v[...].astype(f32), axis=1, keepdims=True)
    lane_of = line % LINES
    weight = jnp.where(lane_of[:, :1] < half, weight, 1.0)
    load_go.wait()
    load_ti.wait()
    block = jnp.zeros((block_rows, wide), f32)
    for g in range(LINES):
        picked = jnp.where(lane_of == g, sel, 0.0).astype(bf16)
        source = go_v if g < half else ti_v
        columns = pl.ds((g % half) * wide, wide)
        block += jnp.dot(picked, source[:, columns], preferred_element_type=f32)
    recv[me] = (block * weight).astype(bf16)
    pl.semaphore_wait(barrier, outer + inner - 1)

    sends = []

    def spread(b, ep):
        copy = to(recv.at[b], recv.at[b], a_send.at[len(sends)], a_recv.at[b], ep, core)
        copy.start()
        sends.append(copy)

    def arrived(b):
        to(recv.at[b], recv.at[b], a_send.at[0], a_recv.at[b], me, partner).wait_recv()

    def unpack(b):
        at = pl.ds(pl.multiple_of(b * block_rows, LINES), block_rows)
        for c in range(wide // LANES):
            x32[c, at, :] = recv[b, :, pl.ds(c * LANES, LANES)].astype(f32)

    for k in range(outer - 1, 0, -1):
        spread(me, ((o + k) % outer) * inner + i)
    for j in range(1, inner):
        spread(me, o * inner + (i + j) % inner)
    push_wi = to(w_in, wi_v.at[mine], w_send.at[0], w_recv.at[0], me, partner)
    push_wo = to(w_out, wo_v.at[mine], w_send.at[1], w_recv.at[1], me, partner)
    push_wi.start()
    push_wo.start()
    unpack(me)
    for k in range(1, outer):
        b = ((o + outer - k) % outer) * inner + i
        arrived(b)
        for j in range(1, inner):
            spread(b, o * inner + (i + j) % inner)
        unpack(b)
    load_wi.wait()
    load_wo.wait()
    to(w_in, wi_v.at[theirs], w_send.at[0], w_recv.at[0], me, partner).wait_recv()
    to(w_out, wo_v.at[theirs], w_send.at[1], w_recv.at[1], me, partner).wait_recv()
    for k in range(outer):
        for j in range(1, inner):
            b = ((o + outer - k) % outer) * inner + (i + inner - j) % inner
            arrived(b)
            unpack(b)

    for g in range(LINES):
        dest = q_b if g < half else x_b
        for c in range(wide // LANES):
            columns = pl.ds((g % half) * wide + c * LANES, LANES)
            dest[:, columns] = x32[c, pl.ds(g, slots, stride=LINES), :].astype(bf16)

    last = (((1,), (1,)), ((), ()))
    pre = lax.dot_general(wi_v[...], x_b[...], last, preferred_element_type=f32)
    back = lax.dot_general(wo_v[...], q_b[...], last, preferred_element_type=f32)
    sig = jax.nn.sigmoid(pre)
    grad_pre = back * sig * (1.0 + pre * (1.0 - sig))
    gp_v[...] = grad_pre.astype(bf16)
    hid_v[...] = (pre * sig).astype(bf16)
    flat = grad_pre.T.astype(bf16)
    for g in range(LINES):
        piece = jnp.dot(flat, wi_v[:, pl.ds(g * narrow, narrow)], preferred_element_type=f32)
        for c in range(narrow // LANES):
            ret32[c, pl.ds(g, slots, stride=LINES), :] = piece[:, c * LANES : (c + 1) * LANES]
    for b in range(n):
        for c in range(narrow // LANES):
            ret_send[b, :, pl.ds(c * LANES, LANES)] = ret32[
                c, pl.ds(b * block_rows, block_rows), :
            ].astype(bf16)
    returns = []
    for k in range(n - 1, 0, -1):
        dst = (me + k) % n
        copy = to(ret_send.at[dst], ret_recv.at[me], r_send.at[k - 1], r_recv.at[me], dst, core)
        copy.start()
        returns.append(copy)

    chunk = 512
    swaps = []
    for w, (left, right) in enumerate(((gp_v, x_b), (hid_v, q_b))):
        for c in range(0, width, chunk):
            cols = pl.ds(c, chunk)
            d_send[w, :, cols] = jnp.dot(
                left[theirs, :], right[:, cols], preferred_element_type=f32
            ).astype(bf16)
        copy = to(d_send.at[w], d_recv.at[w], d_ssem.at[w], d_rsem.at[w], me, partner)
        copy.start()
        swaps.append(copy)
    grad_scale = 1.0 / math.sqrt(2 * slots)
    for w, (left, right) in enumerate(((gp_v, x_b), (hid_v, q_b))):
        swaps[w].wait_recv()
        for c in range(0, width, chunk):
            cols = pl.ds(c, chunk)
            own = jnp.dot(left[mine, :], right[:, cols], preferred_element_type=f32)
            total = own.astype(bf16).astype(f32) + d_recv[w, :, cols].astype(f32)
            grads_out[w, :, cols] = (total * grad_scale).astype(bf16)

    summed = ret_send[me].astype(f32)
    for k in range(1, n):
        b = (me + n - k) % n
        to(ret_send.at[b], ret_recv.at[b], r_send.at[0], r_recv.at[b], me, partner).wait_recv()
        summed += ret_recv[b].astype(f32)
    rounded = summed.astype(bf16)
    for g in range(LINES):
        picked = jnp.where(lane_of == g, sel, 0.0).T.astype(bf16)
        tok_out[:, pl.ds(g * narrow, narrow)] = jnp.dot(
            picked, rounded, preferred_element_type=f32
        ).astype(bf16)
    for copy in sends + returns + swaps + [push_wi, push_wo]:
        copy.wait_send()


def write_kernel(tok_grad, grads, tok_out, gin_out, gout_out, sem):
    copies = (
        pltpu.make_async_copy(grads.at[0], gin_out, sem.at[0]),
        pltpu.make_async_copy(grads.at[1], gout_out, sem.at[1]),
        pltpu.make_async_copy(tok_grad, tok_out, sem.at[2]),
    )
    for copy in copies:
        copy.start()
    for copy in copies:
        copy.wait()


def per_device_fused(grad_out, router_prob, routes, token_inputs, w_in, w_out):
    n = lax.axis_size("ep")
    inner = 1 << (n.bit_length() // 2)
    tok_rows, width = token_inputs.shape
    rows = w_in.shape[0]
    block_rows = CAP * LINES
    wide = 2 * width // LINES
    narrow = width // LINES
    slots = n * CAP
    f32, bf16 = jnp.float32, jnp.bfloat16
    copies = n - 1
    dma = pltpu.SemaphoreType.DMA
    hbm = pl.BlockSpec(memory_space=pltpu.HBM)
    vmem = pl.BlockSpec(memory_space=pltpu.VMEM)
    tok_grad, grads = pl.pallas_call(
        functools.partial(fused_kernel, n, inner),
        out_shape=(
            pltpu.VMEM((tok_rows, width), bf16),
            pltpu.VMEM((2, rows, width), bf16),
        ),
        in_specs=[hbm] * 6,
        out_specs=(vmem, vmem),
        scratch_shapes=[
            pltpu.VMEM((tok_rows, width), bf16),
            pltpu.VMEM((tok_rows, width), bf16),
            pltpu.VMEM((2 * rows, width), bf16),
            pltpu.VMEM((2 * rows, width), bf16),
            pltpu.VMEM((n, block_rows, wide), bf16),
            pltpu.VMEM((wide // LANES, n * block_rows, LANES), f32),
            pltpu.VMEM((slots, width), bf16),
            pltpu.VMEM((slots, width), bf16),
            pltpu.VMEM((2 * rows, slots), bf16),
            pltpu.VMEM((2 * rows, slots), bf16),
            pltpu.VMEM((narrow // LANES, n * block_rows, LANES), f32),
            pltpu.VMEM((n, block_rows, narrow), bf16),
            pltpu.VMEM((n, block_rows, narrow), bf16),
            pltpu.VMEM((2, rows, width), bf16),
            pltpu.VMEM((2, rows, width), bf16),
            pltpu.VMEM((1, tok_rows), bf16),
            pltpu.VMEM((1, tok_rows), jnp.int32),
            dma((6,)),
            dma((2,)),
            dma((2,)),
            dma((copies,)),
            dma((n,)),
            dma((copies,)),
            dma((n,)),
            dma((2,)),
            dma((2,)),
        ],
        compiler_params=pltpu.CompilerParams(
            collective_id=0, has_side_effects=True, vmem_limit_bytes=63_000_000
        ),
    )(grad_out, router_prob.reshape(1, tok_rows), routes.reshape(1, tok_rows), token_inputs, w_in, w_out)
    return pl.pallas_call(
        write_kernel,
        out_shape=(
            jax.ShapeDtypeStruct((tok_rows, width), bf16),
            jax.ShapeDtypeStruct((rows, width), bf16),
            jax.ShapeDtypeStruct((rows, width), bf16),
        ),
        in_specs=[vmem, vmem],
        out_specs=(hbm, hbm, hbm),
        scratch_shapes=[dma((3,))],
        compiler_params=pltpu.CompilerParams(vmem_limit_bytes=8 * 1024 * 1024),
    )(tok_grad, grads)


def solution(mesh):
    in_specs = (
        P(("ep", "dp"), None),
        P(("ep", "dp")),
        P(("ep", "dp"), None),
        P(("ep", "dp"), None),
        P(("ep", "dp"), None),
        P(("ep", "dp"), None),
    )
    out_specs = (P(("ep", "dp"), None), P(("ep", "dp"), None), P(("ep", "dp"), None))
    fused = mesh.shape["ep"] == GROUP and mesh.shape["dp"] == 2
    return jax.shard_map(
        per_device_fused if fused else per_device, mesh=mesh, in_specs=in_specs, out_specs=out_specs, check_vma=False
    )
```

```python
import functools
import math

import jax
import jax.numpy as jnp
from jax import lax
from jax.experimental import pallas as pl
from jax.experimental.pallas import tpu as pltpu
from jax.sharding import PartitionSpec as P

GROUP = 16
CAP = 3
LINES = 8
LANES = 128
MESH = pl.DeviceIdType.MESH


def per_device(grad_out, router_prob, routes, token_inputs, w_in, w_out):
    ep_count = lax.axis_size("ep")
    replicas = lax.axis_size("dp")
    flight = ep_count // GROUP
    tok_rows = grad_out.shape[0]
    model_width = grad_out.shape[1]
    expert_ids = routes[:, 0]
    in_window = expert_ids < flight
    onehot = (expert_ids[:, None] == jnp.arange(flight, dtype=jnp.int32)[None, :]).astype(
        jnp.bfloat16
    )
    earlier = (
        jnp.arange(tok_rows, dtype=jnp.int32)[:, None]
        > jnp.arange(tok_rows, dtype=jnp.int32)[None, :]
    ).astype(jnp.bfloat16)
    before = jnp.dot(earlier, onehot, preferred_element_type=jnp.float32)
    slot_rank = jnp.sum(before * onehot.astype(jnp.float32), axis=1).astype(jnp.int32)
    window_rows = flight * CAP
    target = jnp.where(in_window, expert_ids * CAP + slot_rank, window_rows)
    chooser = (jnp.arange(window_rows, dtype=jnp.int32)[:, None] == target[None, :]).astype(
        jnp.bfloat16
    )
    scaled = (router_prob.astype(jnp.float32)[:, None] * grad_out.astype(jnp.float32)).astype(
        jnp.bfloat16
    )
    paired = jnp.concatenate((scaled, token_inputs), axis=1)
    outgoing = jnp.dot(chooser, paired, preferred_element_type=jnp.float32).astype(jnp.bfloat16)
    outgoing = jnp.broadcast_to(
        outgoing.reshape(flight, 1, CAP, 2 * model_width), (flight, GROUP, CAP, 2 * model_width)
    )
    outgoing = outgoing.reshape(ep_count, CAP, 2 * model_width)
    incoming = lax.all_to_all(outgoing, "ep", split_axis=0, concat_axis=0, tiled=True)
    slot_total = ep_count * CAP
    incoming = incoming.reshape(slot_total, 2 * model_width)
    cotangent = incoming[:, :model_width]
    rows_in = incoming[:, model_width:]
    weight_in, weight_out = (
        lax.all_gather(w_in, "dp", axis=0, tiled=True),
        lax.all_gather(w_out, "dp", axis=0, tiled=True),
    )
    contract_last = (((1,), (1,)), ((), ()))
    contract_first = (((0,), (0,)), ((), ()))
    pre_act = lax.dot_general(rows_in, weight_in, contract_last, preferred_element_type=jnp.float32)
    gate_sig = jax.nn.sigmoid(pre_act)
    hidden = (pre_act * gate_sig).astype(jnp.bfloat16)
    back_prop = lax.dot_general(
        cotangent, weight_out, contract_last, preferred_element_type=jnp.float32
    )
    grad_pre = (back_prop * gate_sig * (1.0 + pre_act * (1.0 - gate_sig))).astype(jnp.bfloat16)
    piece_grad = jnp.dot(grad_pre, weight_in, preferred_element_type=jnp.float32).astype(
        jnp.bfloat16
    )
    piece_grad = piece_grad.reshape(ep_count, CAP, model_width)
    returned = lax.all_to_all(piece_grad, "ep", split_axis=0, concat_axis=0, tiled=True)
    summed = jnp.sum(returned.reshape(flight, GROUP, CAP, model_width).astype(jnp.float32), axis=1)
    summed = summed.reshape(window_rows, model_width)
    picked = jnp.take(summed, jnp.minimum(target, window_rows - 1), axis=0)
    grad_tokens = jnp.where(in_window[:, None], picked, jnp.float32(0.0)).astype(jnp.bfloat16)
    grad_scale = 1.0 / math.sqrt(replicas * slot_total)
    columns = grad_pre
    grad_in = lax.psum_scatter(
        lax.dot_general(
            columns, rows_in, contract_first, preferred_element_type=jnp.float32
        ).astype(jnp.bfloat16),
        "dp",
        scatter_dimension=0,
        tiled=True,
    ).astype(jnp.float32)
    columns = hidden
    grad_outw = lax.psum_scatter(
        lax.dot_general(
            columns, cotangent, contract_first, preferred_element_type=jnp.float32
        ).astype(jnp.bfloat16),
        "dp",
        scatter_dimension=0,
        tiled=True,
    ).astype(jnp.float32)
    return (
        grad_tokens,
        (grad_in * grad_scale).astype(jnp.bfloat16),
        (grad_outw * grad_scale).astype(jnp.bfloat16),
    )


def fused_kernel(
    n,
    inner,
    grad_out,
    prob,
    routes,
    tokens,
    w_in,
    w_out,
    tok_out,
    grads_out,
    go_v,
    ti_v,
    wi_v,
    wo_v,
    recv,
    x32,
    q_b,
    x_b,
    hid_v,
    gp_v,
    ret32,
    ret_send,
    ret_recv,
    d_send,
    d_recv,
    prob_v,
    routes_v,
    load_sem,
    w_send,
    w_recv,
    a_send,
    a_recv,
    r_send,
    r_recv,
    d_ssem,
    d_rsem,
):
    me = lax.axis_index("ep")
    core = lax.axis_index("dp")
    partner = 1 - core
    outer = n // inner
    o, i = me // inner, me % inner
    rows, width = w_in.shape
    tok_rows = tokens.shape[0]
    block_rows = CAP * LINES
    half = LINES // 2
    wide = 2 * width // LINES
    narrow = width // LINES
    slots = n * CAP
    f32, bf16 = jnp.float32, jnp.bfloat16

    def to(src, dst, send, arrive, ep, dp):
        return pltpu.make_async_remote_copy(
            src_ref=src,
            dst_ref=dst,
            send_sem=send,
            recv_sem=arrive,
            device_id=(ep, dp),
            device_id_type=MESH,
        )

    barrier = pltpu.get_barrier_semaphore()
    for k in range(1, outer):
        peer = ((o + k) % outer) * inner + i
        pl.semaphore_signal(barrier, inc=1, device_id=(peer, core), device_id_type=MESH)
    for j in range(1, inner):
        peer = o * inner + (i + j) % inner
        pl.semaphore_signal(barrier, inc=1, device_id=(peer, core), device_id_type=MESH)
    pl.semaphore_signal(barrier, inc=1, device_id=(me, partner), device_id_type=MESH)

    load_go = pltpu.make_async_copy(grad_out, go_v, load_sem.at[0])
    load_ti = pltpu.make_async_copy(tokens, ti_v, load_sem.at[1])
    mine = pl.ds(pl.multiple_of(core * rows, rows), rows)
    theirs = pl.ds(pl.multiple_of(partner * rows, rows), rows)
    load_wi = pltpu.make_async_copy(w_in, wi_v.at[mine], load_sem.at[2])
    load_wo = pltpu.make_async_copy(w_out, wo_v.at[mine], load_sem.at[3])
    load_prob = pltpu.make_async_copy(prob, prob_v, load_sem.at[4])
    load_routes = pltpu.make_async_copy(routes, routes_v, load_sem.at[5])
    load_routes.start()
    load_prob.start()
    load_go.start()
    load_ti.start()
    load_wi.start()
    load_wo.start()

    line = lax.broadcasted_iota(jnp.int32, (block_rows, tok_rows), 0)
    load_routes.wait()
    load_prob.wait()
    in_window = jnp.broadcast_to((routes_v[...] < 1).astype(f32), (block_rows, tok_rows))
    earlier = (
        lax.broadcasted_iota(jnp.int32, (tok_rows, tok_rows), 0)
        < lax.broadcasted_iota(jnp.int32, (tok_rows, tok_rows), 1)
    ).astype(f32).astype(bf16)
    rank = jnp.dot(in_window.astype(bf16), earlier, preferred_element_type=f32)
    rank_of_line = (line // LINES).astype(f32)
    sel = jnp.where(rank == rank_of_line, in_window, 0.0)
    weight = jnp.sum(sel * prob_v[...].astype(f32), axis=1, keepdims=True)
    lane_of = line % LINES
    weight = jnp.where(lane_of[:, :1] < half, weight, 1.0)
    load_go.wait()
    load_ti.wait()
    block = jnp.zeros((block_rows, wide), f32)
    for g in range(LINES):
        picked = jnp.where(lane_of == g, sel, 0.0).astype(bf16)
        source = go_v if g < half else ti_v
        columns = pl.ds((g % half) * wide, wide)
        block += jnp.dot(picked, source[:, columns], preferred_element_type=f32)
    recv[me] = (block * weight).astype(bf16)
    pl.semaphore_wait(barrier, outer + inner - 1)

    sends = []

    def spread(b, ep):
        copy = to(recv.at[b], recv.at[b], a_send.at[len(sends)], a_recv.at[b], ep, core)
        copy.start()
        sends.append(copy)

    def arrived(b):
        to(recv.at[b], recv.at[b], a_send.at[0], a_recv.at[b], me, partner).wait_recv()

    def unpack(b):
        at = pl.ds(pl.multiple_of(b * block_rows, LINES), block_rows)
        for c in range(wide // LANES):
            x32[c, at, :] = recv[b, :, pl.ds(c * LANES, LANES)].astype(f32)

    for k in range(outer - 1, 0, -1):
        spread(me, ((o + k) % outer) * inner + i)
    for j in range(1, inner):
        spread(me, o * inner + (i + j) % inner)
    push_wi = to(w_in, wi_v.at[mine], w_send.at[0], w_recv.at[0], me, partner)
    push_wo = to(w_out, wo_v.at[mine], w_send.at[1], w_recv.at[1], me, partner)
    push_wi.start()
    push_wo.start()
    unpack(me)
    for k in range(1, outer):
        b = ((o + outer - k) % outer) * inner + i
        arrived(b)
        for j in range(1, inner):
            spread(b, o * inner + (i + j) % inner)
        unpack(b)
    load_wi.wait()
    load_wo.wait()
    to(w_in, wi_v.at[theirs], w_send.at[0], w_recv.at[0], me, partner).wait_recv()
    to(w_out, wo_v.at[theirs], w_send.at[1], w_recv.at[1], me, partner).wait_recv()
    for k in range(outer):
        for j in range(1, inner):
            b = ((o + outer - k) % outer) * inner + (i + inner - j) % inner
            arrived(b)
            unpack(b)

    for g in range(LINES):
        dest = q_b if g < half else x_b
        for c in range(wide // LANES):
            columns = pl.ds((g % half) * wide + c * LANES, LANES)
            dest[:, columns] = x32[c, pl.ds(g, slots, stride=LINES), :].astype(bf16)

    last = (((1,), (1,)), ((), ()))
    pre = lax.dot_general(wi_v[...], x_b[...], last, preferred_element_type=f32)
    back = lax.dot_general(wo_v[...], q_b[...], last, preferred_element_type=f32)
    sig = jax.nn.sigmoid(pre)
    grad_pre = back * sig * (1.0 + pre * (1.0 - sig))
    gp_v[...] = grad_pre.astype(bf16)
    hid_v[...] = (pre * sig).astype(bf16)
    flat = grad_pre.T.astype(bf16)
    for g in range(LINES):
        piece = jnp.dot(flat, wi_v[:, pl.ds(g * narrow, narrow)], preferred_element_type=f32)
        for c in range(narrow // LANES):
            ret32[c, pl.ds(g, slots, stride=LINES), :] = piece[:, c * LANES : (c + 1) * LANES]
    for b in range(n):
        for c in range(narrow // LANES):
            ret_send[b, :, pl.ds(c * LANES, LANES)] = ret32[
                c, pl.ds(b * block_rows, block_rows), :
            ].astype(bf16)
    returns = []
    for k in range(1, n):
        dst = (me + k) % n
        copy = to(ret_send.at[dst], ret_recv.at[me], r_send.at[k - 1], r_recv.at[me], dst, core)
        copy.start()
        returns.append(copy)

    chunk = 512
    swaps = []
    for w, (left, right) in enumerate(((gp_v, x_b), (hid_v, q_b))):
        for c in range(0, width, chunk):
            cols = pl.ds(c, chunk)
            d_send[w, :, cols] = jnp.dot(
                left[theirs, :], right[:, cols], preferred_element_type=f32
            ).astype(bf16)
        copy = to(d_send.at[w], d_recv.at[w], d_ssem.at[w], d_rsem.at[w], me, partner)
        copy.start()
        swaps.append(copy)
    grad_scale = 1.0 / math.sqrt(2 * slots)
    for w, (left, right) in enumerate(((gp_v, x_b), (hid_v, q_b))):
        swaps[w].wait_recv()
        for c in range(0, width, chunk):
            cols = pl.ds(c, chunk)
            own = jnp.dot(left[mine, :], right[:, cols], preferred_element_type=f32)
            total = own.astype(bf16).astype(f32) + d_recv[w, :, cols].astype(f32)
            grads_out[w, :, cols] = (total * grad_scale).astype(bf16)

    summed = ret_send[me].astype(f32)
    for k in range(1, n):
        b = (me + n - k) % n
        to(ret_send.at[b], ret_recv.at[b], r_send.at[0], r_recv.at[b], me, partner).wait_recv()
        summed += ret_recv[b].astype(f32)
    rounded = summed.astype(bf16)
    for g in range(LINES):
        picked = jnp.where(lane_of == g, sel, 0.0).T.astype(bf16)
        tok_out[:, pl.ds(g * narrow, narrow)] = jnp.dot(
            picked, rounded, preferred_element_type=f32
        ).astype(bf16)
    for copy in sends + returns + swaps + [push_wi, push_wo]:
        copy.wait_send()


def write_kernel(tok_grad, grads, tok_out, gin_out, gout_out, sem):
    copies = (
        pltpu.make_async_copy(grads.at[0], gin_out, sem.at[0]),
        pltpu.make_async_copy(grads.at[1], gout_out, sem.at[1]),
        pltpu.make_async_copy(tok_grad, tok_out, sem.at[2]),
    )
    for copy in copies:
        copy.start()
    for copy in copies:
        copy.wait()


def per_device_fused(grad_out, router_prob, routes, token_inputs, w_in, w_out):
    n = lax.axis_size("ep")
    inner = 1 << (n.bit_length() // 2)
    tok_rows, width = token_inputs.shape
    rows = w_in.shape[0]
    block_rows = CAP * LINES
    wide = 2 * width // LINES
    narrow = width // LINES
    slots = n * CAP
    f32, bf16 = jnp.float32, jnp.bfloat16
    copies = n - 1
    dma = pltpu.SemaphoreType.DMA
    hbm = pl.BlockSpec(memory_space=pltpu.HBM)
    vmem = pl.BlockSpec(memory_space=pltpu.VMEM)
    tok_grad, grads = pl.pallas_call(
        functools.partial(fused_kernel, n, inner),
        out_shape=(
            pltpu.VMEM((tok_rows, width), bf16),
            pltpu.VMEM((2, rows, width), bf16),
        ),
        in_specs=[hbm] * 6,
        out_specs=(vmem, vmem),
        scratch_shapes=[
            pltpu.VMEM((tok_rows, width), bf16),
            pltpu.VMEM((tok_rows, width), bf16),
            pltpu.VMEM((2 * rows, width), bf16),
            pltpu.VMEM((2 * rows, width), bf16),
            pltpu.VMEM((n, block_rows, wide), bf16),
            pltpu.VMEM((wide // LANES, n * block_rows, LANES), f32),
            pltpu.VMEM((slots, width), bf16),
            pltpu.VMEM((slots, width), bf16),
            pltpu.VMEM((2 * rows, slots), bf16),
            pltpu.VMEM((2 * rows, slots), bf16),
            pltpu.VMEM((narrow // LANES, n * block_rows, LANES), f32),
            pltpu.VMEM((n, block_rows, narrow), bf16),
            pltpu.VMEM((n, block_rows, narrow), bf16),
            pltpu.VMEM((2, rows, width), bf16),
            pltpu.VMEM((2, rows, width), bf16),
            pltpu.VMEM((1, tok_rows), bf16),
            pltpu.VMEM((1, tok_rows), jnp.int32),
            dma((6,)),
            dma((2,)),
            dma((2,)),
            dma((copies,)),
            dma((n,)),
            dma((copies,)),
            dma((n,)),
            dma((2,)),
            dma((2,)),
        ],
        compiler_params=pltpu.CompilerParams(
            collective_id=0, has_side_effects=True, vmem_limit_bytes=63_000_000
        ),
    )(grad_out, router_prob.reshape(1, tok_rows), routes.reshape(1, tok_rows), token_inputs, w_in, w_out)
    return pl.pallas_call(
        write_kernel,
        out_shape=(
            jax.ShapeDtypeStruct((tok_rows, width), bf16),
            jax.ShapeDtypeStruct((rows, width), bf16),
            jax.ShapeDtypeStruct((rows, width), bf16),
        ),
        in_specs=[vmem, vmem],
        out_specs=(hbm, hbm, hbm),
        scratch_shapes=[dma((3,))],
        compiler_params=pltpu.CompilerParams(vmem_limit_bytes=8 * 1024 * 1024),
    )(tok_grad, grads)


def solution(mesh):
    in_specs = (
        P(("ep", "dp"), None),
        P(("ep", "dp")),
        P(("ep", "dp"), None),
        P(("ep", "dp"), None),
        P(("ep", "dp"), None),
        P(("ep", "dp"), None),
    )
    out_specs = (P(("ep", "dp"), None), P(("ep", "dp"), None), P(("ep", "dp"), None))
    fused = mesh.shape["ep"] == GROUP and mesh.shape["dp"] == 2
    return jax.shard_map(
        per_device_fused if fused else per_device, mesh=mesh, in_specs=in_specs, out_specs=out_specs, check_vma=False
    )
```

```python
import functools
import math

import jax
import jax.numpy as jnp
from jax import lax
from jax.experimental import pallas as pl
from jax.experimental.pallas import tpu as pltpu
from jax.sharding import PartitionSpec as P

GROUP = 16
CAP = 3
LINES = 8
LANES = 128
MESH = pl.DeviceIdType.MESH


def per_device(grad_out, router_prob, routes, token_inputs, w_in, w_out):
    ep_count = lax.axis_size("ep")
    replicas = lax.axis_size("dp")
    flight = ep_count // GROUP
    tok_rows = grad_out.shape[0]
    model_width = grad_out.shape[1]
    expert_ids = routes[:, 0]
    in_window = expert_ids < flight
    onehot = (expert_ids[:, None] == jnp.arange(flight, dtype=jnp.int32)[None, :]).astype(
        jnp.bfloat16
    )
    earlier = (
        jnp.arange(tok_rows, dtype=jnp.int32)[:, None]
        > jnp.arange(tok_rows, dtype=jnp.int32)[None, :]
    ).astype(jnp.bfloat16)
    before = jnp.dot(earlier, onehot, preferred_element_type=jnp.float32)
    slot_rank = jnp.sum(before * onehot.astype(jnp.float32), axis=1).astype(jnp.int32)
    window_rows = flight * CAP
    target = jnp.where(in_window, expert_ids * CAP + slot_rank, window_rows)
    chooser = (jnp.arange(window_rows, dtype=jnp.int32)[:, None] == target[None, :]).astype(
        jnp.bfloat16
    )
    scaled = (router_prob.astype(jnp.float32)[:, None] * grad_out.astype(jnp.float32)).astype(
        jnp.bfloat16
    )
    paired = jnp.concatenate((scaled, token_inputs), axis=1)
    outgoing = jnp.dot(chooser, paired, preferred_element_type=jnp.float32).astype(jnp.bfloat16)
    outgoing = jnp.broadcast_to(
        outgoing.reshape(flight, 1, CAP, 2 * model_width), (flight, GROUP, CAP, 2 * model_width)
    )
    outgoing = outgoing.reshape(ep_count, CAP, 2 * model_width)
    incoming = lax.all_to_all(outgoing, "ep", split_axis=0, concat_axis=0, tiled=True)
    slot_total = ep_count * CAP
    incoming = incoming.reshape(slot_total, 2 * model_width)
    cotangent = incoming[:, :model_width]
    rows_in = incoming[:, model_width:]
    weight_in, weight_out = (
        lax.all_gather(w_in, "dp", axis=0, tiled=True),
        lax.all_gather(w_out, "dp", axis=0, tiled=True),
    )
    contract_last = (((1,), (1,)), ((), ()))
    contract_first = (((0,), (0,)), ((), ()))
    pre_act = lax.dot_general(rows_in, weight_in, contract_last, preferred_element_type=jnp.float32)
    gate_sig = jax.nn.sigmoid(pre_act)
    hidden = (pre_act * gate_sig).astype(jnp.bfloat16)
    back_prop = lax.dot_general(
        cotangent, weight_out, contract_last, preferred_element_type=jnp.float32
    )
    grad_pre = (back_prop * gate_sig * (1.0 + pre_act * (1.0 - gate_sig))).astype(jnp.bfloat16)
    piece_grad = jnp.dot(grad_pre, weight_in, preferred_element_type=jnp.float32).astype(
        jnp.bfloat16
    )
    piece_grad = piece_grad.reshape(ep_count, CAP, model_width)
    returned = lax.all_to_all(piece_grad, "ep", split_axis=0, concat_axis=0, tiled=True)
    summed = jnp.sum(returned.reshape(flight, GROUP, CAP, model_width).astype(jnp.float32), axis=1)
    summed = summed.reshape(window_rows, model_width)
    picked = jnp.take(summed, jnp.minimum(target, window_rows - 1), axis=0)
    grad_tokens = jnp.where(in_window[:, None], picked, jnp.float32(0.0)).astype(jnp.bfloat16)
    grad_scale = 1.0 / math.sqrt(replicas * slot_total)
    columns = grad_pre
    grad_in = lax.psum_scatter(
        lax.dot_general(
            columns, rows_in, contract_first, preferred_element_type=jnp.float32
        ).astype(jnp.bfloat16),
        "dp",
        scatter_dimension=0,
        tiled=True,
    ).astype(jnp.float32)
    columns = hidden
    grad_outw = lax.psum_scatter(
        lax.dot_general(
            columns, cotangent, contract_first, preferred_element_type=jnp.float32
        ).astype(jnp.bfloat16),
        "dp",
        scatter_dimension=0,
        tiled=True,
    ).astype(jnp.float32)
    return (
        grad_tokens,
        (grad_in * grad_scale).astype(jnp.bfloat16),
        (grad_outw * grad_scale).astype(jnp.bfloat16),
    )


def fused_kernel(
    n,
    inner,
    grad_out,
    prob,
    routes,
    tokens,
    w_in,
    w_out,
    tok_out,
    grads_out,
    go_v,
    ti_v,
    wi_v,
    wo_v,
    recv,
    x32,
    q_b,
    x_b,
    hid_v,
    gp_v,
    ret32,
    ret_send,
    ret_recv,
    d_send,
    d_recv,
    prob_v,
    routes_v,
    load_sem,
    w_send,
    w_recv,
    a_send,
    a_recv,
    r_send,
    r_recv,
    d_ssem,
    d_rsem,
):
    me = lax.axis_index("ep")
    core = lax.axis_index("dp")
    partner = 1 - core
    outer = n // inner
    o, i = me // inner, me % inner
    rows, width = w_in.shape
    tok_rows = tokens.shape[0]
    block_rows = CAP * LINES
    half = LINES // 2
    wide = 2 * width // LINES
    narrow = width // LINES
    slots = n * CAP
    f32, bf16 = jnp.float32, jnp.bfloat16

    def to(src, dst, send, arrive, ep, dp):
        return pltpu.make_async_remote_copy(
            src_ref=src,
            dst_ref=dst,
            send_sem=send,
            recv_sem=arrive,
            device_id=(ep, dp),
            device_id_type=MESH,
        )

    barrier = pltpu.get_barrier_semaphore()
    for k in range(1, outer):
        peer = ((o + k) % outer) * inner + i
        pl.semaphore_signal(barrier, inc=1, device_id=(peer, core), device_id_type=MESH)
    for j in range(1, inner):
        peer = o * inner + (i + j) % inner
        pl.semaphore_signal(barrier, inc=1, device_id=(peer, core), device_id_type=MESH)
    pl.semaphore_signal(barrier, inc=1, device_id=(me, partner), device_id_type=MESH)

    load_go = pltpu.make_async_copy(grad_out, go_v, load_sem.at[0])
    load_ti = pltpu.make_async_copy(tokens, ti_v, load_sem.at[1])
    mine = pl.ds(pl.multiple_of(core * rows, rows), rows)
    theirs = pl.ds(pl.multiple_of(partner * rows, rows), rows)
    load_wi = pltpu.make_async_copy(w_in, wi_v.at[mine], load_sem.at[2])
    load_wo = pltpu.make_async_copy(w_out, wo_v.at[mine], load_sem.at[3])
    load_prob = pltpu.make_async_copy(prob, prob_v, load_sem.at[4])
    load_routes = pltpu.make_async_copy(routes, routes_v, load_sem.at[5])
    load_routes.start()
    load_prob.start()
    load_go.start()
    load_ti.start()
    load_wi.start()
    load_wo.start()

    line = lax.broadcasted_iota(jnp.int32, (block_rows, tok_rows), 0)
    load_routes.wait()
    load_prob.wait()
    in_window = jnp.broadcast_to((routes_v[...] < 1).astype(f32), (block_rows, tok_rows))
    earlier = (
        lax.broadcasted_iota(jnp.int32, (tok_rows, tok_rows), 0)
        < lax.broadcasted_iota(jnp.int32, (tok_rows, tok_rows), 1)
    ).astype(f32).astype(bf16)
    rank = jnp.dot(in_window.astype(bf16), earlier, preferred_element_type=f32)
    rank_of_line = (line // LINES).astype(f32)
    sel = jnp.where(rank == rank_of_line, in_window, 0.0)
    weight = jnp.sum(sel * prob_v[...].astype(f32), axis=1, keepdims=True)
    lane_of = line % LINES
    weight = jnp.where(lane_of[:, :1] < half, weight, 1.0)
    load_go.wait()
    load_ti.wait()
    block = jnp.zeros((block_rows, wide), f32)
    for g in range(LINES):
        picked = jnp.where(lane_of == g, sel, 0.0).astype(bf16)
        source = go_v if g < half else ti_v
        columns = pl.ds((g % half) * wide, wide)
        block += jnp.dot(picked, source[:, columns], preferred_element_type=f32)
    recv[me] = (block * weight).astype(bf16)
    pl.semaphore_wait(barrier, outer + inner - 1)

    sends = []

    def spread(b, ep):
        copy = to(recv.at[b], recv.at[b], a_send.at[len(sends)], a_recv.at[b], ep, core)
        copy.start()
        sends.append(copy)

    def arrived(b):
        to(recv.at[b], recv.at[b], a_send.at[0], a_recv.at[b], me, partner).wait_recv()

    def unpack(b):
        at = pl.ds(pl.multiple_of(b * block_rows, LINES), block_rows)
        for c in range(wide // LANES):
            x32[c, at, :] = recv[b, :, pl.ds(c * LANES, LANES)].astype(f32)

    for k in range(1, outer):
        spread(me, ((o + k) % outer) * inner + i)
    for j in range(1, inner):
        spread(me, o * inner + (i + j) % inner)
    push_wi = to(w_in, wi_v.at[mine], w_send.at[0], w_recv.at[0], me, partner)
    push_wo = to(w_out, wo_v.at[mine], w_send.at[1], w_recv.at[1], me, partner)
    push_wi.start()
    push_wo.start()
    unpack(me)
    for k in range(1, outer):
        b = ((o + outer - k) % outer) * inner + i
        arrived(b)
        for j in range(1, inner):
            spread(b, o * inner + (i + j) % inner)
        unpack(b)
    load_wi.wait()
    load_wo.wait()
    to(w_in, wi_v.at[theirs], w_send.at[0], w_recv.at[0], me, partner).wait_recv()
    to(w_out, wo_v.at[theirs], w_send.at[1], w_recv.at[1], me, partner).wait_recv()
    for k in range(outer):
        for j in range(1, inner):
            b = ((o + outer - k) % outer) * inner + (i + inner - j) % inner
            arrived(b)
            unpack(b)

    for g in range(LINES):
        dest = q_b if g < half else x_b
        for c in range(wide // LANES):
            columns = pl.ds((g % half) * wide + c * LANES, LANES)
            dest[:, columns] = x32[c, pl.ds(g, slots, stride=LINES), :].astype(bf16)

    last = (((1,), (1,)), ((), ()))
    pre = lax.dot_general(wi_v[...], x_b[...], last, preferred_element_type=f32)
    back = lax.dot_general(wo_v[...], q_b[...], last, preferred_element_type=f32)
    sig = jax.nn.sigmoid(pre)
    grad_pre = back * sig * (1.0 + pre * (1.0 - sig))
    gp_v[...] = grad_pre.astype(bf16)
    hid_v[...] = (pre * sig).astype(bf16)
    flat = grad_pre.T.astype(bf16)
    for g in range(LINES):
        piece = jnp.dot(flat, wi_v[:, pl.ds(g * narrow, narrow)], preferred_element_type=f32)
        for c in range(narrow // LANES):
            ret32[c, pl.ds(g, slots, stride=LINES), :] = piece[:, c * LANES : (c + 1) * LANES]
    for b in range(n):
        for c in range(narrow // LANES):
            ret_send[b, :, pl.ds(c * LANES, LANES)] = ret32[
                c, pl.ds(b * block_rows, block_rows), :
            ].astype(bf16)
    returns = []
    for k in range(1, n):
        dst = (me + k) % n
        copy = to(ret_send.at[dst], ret_recv.at[me], r_send.at[k - 1], r_recv.at[me], dst, core)
        copy.start()
        returns.append(copy)

    chunk = 512
    swaps = []
    for w, (left, right) in enumerate(((gp_v, x_b), (hid_v, q_b))):
        for c in range(0, width, chunk):
            cols = pl.ds(c, chunk)
            d_send[w, :, cols] = jnp.dot(
                left[theirs, :], right[:, cols], preferred_element_type=f32
            ).astype(bf16)
        copy = to(d_send.at[w], d_recv.at[w], d_ssem.at[w], d_rsem.at[w], me, partner)
        copy.start()
        swaps.append(copy)
    grad_scale = 1.0 / math.sqrt(2 * slots)
    for w, (left, right) in enumerate(((gp_v, x_b), (hid_v, q_b))):
        swaps[w].wait_recv()
        for c in range(0, width, chunk):
            cols = pl.ds(c, chunk)
            own = jnp.dot(left[mine, :], right[:, cols], preferred_element_type=f32)
            total = own.astype(bf16).astype(f32) + d_recv[w, :, cols].astype(f32)
            grads_out[w, :, cols] = (total * grad_scale).astype(bf16)

    summed = ret_send[me].astype(f32)
    for k in range(1, n):
        b = (me + n - k) % n
        to(ret_send.at[b], ret_recv.at[b], r_send.at[0], r_recv.at[b], me, partner).wait_recv()
        summed += ret_recv[b].astype(f32)
    rounded = summed.astype(bf16)
    for g in range(LINES):
        picked = jnp.where(lane_of == g, sel, 0.0).T.astype(bf16)
        tok_out[:, pl.ds(g * narrow, narrow)] = jnp.dot(
            picked, rounded, preferred_element_type=f32
        ).astype(bf16)
    for copy in sends + returns + swaps + [push_wi, push_wo]:
        copy.wait_send()


def write_kernel(tok_grad, grads, tok_out, gin_out, gout_out, sem):
    copies = (
        pltpu.make_async_copy(grads.at[0], gin_out, sem.at[0]),
        pltpu.make_async_copy(grads.at[1], gout_out, sem.at[1]),
        pltpu.make_async_copy(tok_grad, tok_out, sem.at[2]),
    )
    for copy in copies:
        copy.start()
    for copy in copies:
        copy.wait()


def per_device_fused(grad_out, router_prob, routes, token_inputs, w_in, w_out):
    n = lax.axis_size("ep")
    inner = 1 << (n.bit_length() // 2)
    tok_rows, width = token_inputs.shape
    rows = w_in.shape[0]
    block_rows = CAP * LINES
    wide = 2 * width // LINES
    narrow = width // LINES
    slots = n * CAP
    f32, bf16 = jnp.float32, jnp.bfloat16
    copies = n - 1
    dma = pltpu.SemaphoreType.DMA
    hbm = pl.BlockSpec(memory_space=pltpu.HBM)
    vmem = pl.BlockSpec(memory_space=pltpu.VMEM)
    tok_grad, grads = pl.pallas_call(
        functools.partial(fused_kernel, n, inner),
        out_shape=(
            pltpu.VMEM((tok_rows, width), bf16),
            pltpu.VMEM((2, rows, width), bf16),
        ),
        in_specs=[hbm] * 6,
        out_specs=(vmem, vmem),
        scratch_shapes=[
            pltpu.VMEM((tok_rows, width), bf16),
            pltpu.VMEM((tok_rows, width), bf16),
            pltpu.VMEM((2 * rows, width), bf16),
            pltpu.VMEM((2 * rows, width), bf16),
            pltpu.VMEM((n, block_rows, wide), bf16),
            pltpu.VMEM((wide // LANES, n * block_rows, LANES), f32),
            pltpu.VMEM((slots, width), bf16),
            pltpu.VMEM((slots, width), bf16),
            pltpu.VMEM((2 * rows, slots), bf16),
            pltpu.VMEM((2 * rows, slots), bf16),
            pltpu.VMEM((narrow // LANES, n * block_rows, LANES), f32),
            pltpu.VMEM((n, block_rows, narrow), bf16),
            pltpu.VMEM((n, block_rows, narrow), bf16),
            pltpu.VMEM((2, rows, width), bf16),
            pltpu.VMEM((2, rows, width), bf16),
            pltpu.VMEM((1, tok_rows), bf16),
            pltpu.VMEM((1, tok_rows), jnp.int32),
            dma((6,)),
            dma((2,)),
            dma((2,)),
            dma((copies,)),
            dma((n,)),
            dma((copies,)),
            dma((n,)),
            dma((2,)),
            dma((2,)),
        ],
        compiler_params=pltpu.CompilerParams(
            collective_id=0, has_side_effects=True, vmem_limit_bytes=63_000_000
        ),
    )(grad_out, router_prob.reshape(1, tok_rows), routes.reshape(1, tok_rows), token_inputs, w_in, w_out)
    return pl.pallas_call(
        write_kernel,
        out_shape=(
            jax.ShapeDtypeStruct((tok_rows, width), bf16),
            jax.ShapeDtypeStruct((rows, width), bf16),
            jax.ShapeDtypeStruct((rows, width), bf16),
        ),
        in_specs=[vmem, vmem],
        out_specs=(hbm, hbm, hbm),
        scratch_shapes=[dma((3,))],
        compiler_params=pltpu.CompilerParams(vmem_limit_bytes=8 * 1024 * 1024),
    )(tok_grad, grads)


def solution(mesh):
    in_specs = (
        P(("ep", "dp"), None),
        P(("ep", "dp")),
        P(("ep", "dp"), None),
        P(("ep", "dp"), None),
        P(("ep", "dp"), None),
        P(("ep", "dp"), None),
    )
    out_specs = (P(("ep", "dp"), None), P(("ep", "dp"), None), P(("ep", "dp"), None))
    fused = mesh.shape["ep"] == GROUP and mesh.shape["dp"] == 2
    return jax.shard_map(
        per_device_fused if fused else per_device, mesh=mesh, in_specs=in_specs, out_specs=out_specs, check_vma=False
    )
```
